32 devices in a mesh: row: 4 (over z), col: 8 (over y, x, core).
Axes of the slice: x: 2, y: 2, z: 4, core: 2. Of those that a mesh axis runs over, the one named last changes fastest.
Arguments:
- pencil_a: float32 [4, 3072, 8, 1536], P('row', None, 'col'), may hold values from -6 to 6, as said below
- pencil_b: float32 [4, 3072, 8, 1536], P('row', None, 'col'), may hold values from -6 to 6
Outputs:
- new_a: float32 [4, 3072, 8, 1536], P('row', None, 'col')
- new_b: float32 [4, 3072, 8, 1536], P('row', None, 'col')
The draws below stay inside these ranges and needn't reach their ends.
Inputs may be any that keep to these rules, and one draw needn't show every extreme that they name: `pencil_a`: the first 256 columns of Amat are zero in the last 256 rows of Amat.
All inputs are finite; a program needn't handle non-finite values.
Results may differ from the reference program's by a relative error of at most 0.000056.
Values sent between devices are 32-bit elements; how exact they have to be, the bound alone decides.
A program may use at most 192 MiB of HBM per device.

```python
import math
import jax
import jax.numpy as jnp
from jax import lax

N = 12288
NB = 256
N_ROW = 4
N_COL = 8


decay_ratio = 3.0


def to_storage(matrix):
    six = matrix.reshape(N // (NB * N_ROW), N_ROW, NB, N // (NB * N_COL), N_COL, NB)
    return six.transpose(1, 0, 2, 4, 3, 5).reshape(N_ROW, N // N_ROW, N_COL, N // N_COL)


def base_field(key):
    return jax.random.normal(key, (N, N), jnp.float32)


def decay_scales():
    fraction = jnp.arange(NB, dtype=jnp.float32) / (NB - 1)
    return jnp.exp(-math.log(decay_ratio) * fraction)


def reflect_columns(block, key):
    direction = jax.random.normal(key, (NB,), jnp.float32)
    direction = direction / jnp.sqrt(jnp.sum(direction * direction))
    along = jnp.dot(block, direction, precision=lax.Precision.HIGHEST)
    return block - 2.0 * jnp.outer(along, direction)


def draw_pencil_a(key, part):
    inner_key = jax.random.fold_in(key, 11)
    field_key, first_key, second_key = jax.random.split(inner_key, 3)
    matrix = base_field(field_key)
    panel = matrix[:, :NB] * decay_scales()[None, :]
    panel = reflect_columns(panel, first_key)
    panel = reflect_columns(panel, second_key)
    kept_rows = (jnp.arange(N) < N - NB).astype(jnp.float32)[:, None]
    matrix = matrix.at[:, :NB].set(panel * kept_rows)
    return to_storage(jnp.clip(matrix, -6.0, 6.0))


def draw_pencil_b(key, part):
    inner_key = jax.random.fold_in(key, 23)
    field_key, first_key, second_key = jax.random.split(inner_key, 3)
    matrix = base_field(field_key)
    strip_rows = matrix[N - NB:, :] * decay_scales()[:, None]
    mixed_t = reflect_columns(strip_rows.T, first_key)
    mixed_t = reflect_columns(mixed_t, second_key)
    matrix = matrix.at[N - NB:, :].set(mixed_t.T)
    return to_storage(jnp.clip(matrix, -6.0, 6.0))


def setup_inputs(seed: int = 0) -> dict:
    key_list = jax.random.split(jax.random.key(seed), 3)
    pencil_a = draw_pencil_a(jax.random.fold_in(key_list[2], 71), 0)
    pencil_b = draw_pencil_b(jax.random.fold_in(key_list[2], 71), 0)
    return dict(pencil_a=pencil_a, pencil_b=pencil_b)


def matmul(left, right):
    return jnp.dot(left.astype(jnp.float32), right.astype(jnp.float32), precision=lax.Precision.HIGHEST, preferred_element_type=jnp.float32)

def inverse_factor(gram):
    lower = jnp.linalg.cholesky(gram)
    ident = jnp.eye(gram.shape[0], dtype=jnp.float32)
    return jax.scipy.linalg.solve_triangular(lower, ident, lower=True).T

def general_inverse(square):
    lower = jnp.linalg.cholesky(matmul(square, square.T))
    ident = jnp.eye(square.shape[0], dtype=jnp.float32)
    linv = jax.scipy.linalg.solve_triangular(lower, ident, lower=True)
    return matmul(square.T, matmul(linv.T, linv))

def to_matrix(stored):
    six = stored.reshape(N_ROW, N // (NB * N_ROW), NB, N_COL, N // (NB * N_COL), NB)
    return six.transpose(1, 0, 2, 4, 3, 5).reshape(N, N)

def to_stored(matrix):
    six = matrix.reshape(N // (NB * N_ROW), N_ROW, NB, N // (NB * N_COL), N_COL, NB)
    return six.transpose(1, 0, 2, 4, 3, 5).reshape(N_ROW, N // N_ROW, N_COL, N // N_COL)

def reference(pencil_a, pencil_b):
    amat = to_matrix(pencil_a)
    bmat = to_matrix(pencil_b)
    ident = jnp.eye(NB, dtype=jnp.float32)
    panel = amat[:, :NB]
    first_inv = inverse_factor(matmul(panel.T, panel))
    basis = matmul(panel, first_inv)
    kinv_left = general_inverse(ident + basis[:NB])
    vectors = basis.at[:NB].add(ident)
    amat = amat - matmul(vectors, matmul(kinv_left, matmul(vectors.T, amat)))
    bmat = bmat - matmul(vectors, matmul(kinv_left, matmul(vectors.T, bmat)))
    strip = bmat[N - NB:]
    first_inv = inverse_factor(matmul(strip, strip.T))
    basis_t = matmul(first_inv.T, strip)
    kinv_right = general_inverse(ident + basis_t[:, N - NB:].T)
    vectors_t = basis_t.at[:, N - NB:].add(ident)
    amat = amat - matmul(matmul(matmul(amat, vectors_t.T), kinv_right.T), vectors_t)
    bmat = bmat - matmul(matmul(matmul(bmat, vectors_t.T), kinv_right.T), vectors_t)
    return (to_stored(amat), to_stored(bmat))
```

```python
import jax
import jax.numpy as jnp
from jax import lax
from jax.sharding import PartitionSpec as P

NB = 256


def broadcast(array, axis, root):
    mine = lax.axis_index(axis) == root
    return lax.psum(jnp.where(mine, array, jnp.zeros_like(array)), axis)


def matmul(left, right):
    return jnp.dot(left, right, precision=lax.Precision.HIGHEST, preferred_element_type=jnp.float32)


def inverse_factor(gram):
    lower = jnp.linalg.cholesky(gram)
    ident = jnp.eye(gram.shape[0], dtype=jnp.float32)
    return jax.scipy.linalg.solve_triangular(lower, ident, lower=True).T


def general_inverse(square):
    lower = jnp.linalg.cholesky(matmul(square, square.T))
    ident = jnp.eye(square.shape[0], dtype=jnp.float32)
    linv = jax.scipy.linalg.solve_triangular(lower, ident, lower=True)
    return matmul(square.T, matmul(linv.T, linv))


def fast_matmul(left, right):
    return jnp.dot(left, right, precision=lax.Precision.HIGH, preferred_element_type=jnp.float32)


def on_device(pencil_a, pencil_b):
    rows_loc = pencil_a.shape[1]
    cols_loc = pencil_a.shape[3]
    amat = pencil_a.reshape(rows_loc, cols_loc)
    bmat = pencil_b.reshape(rows_loc, cols_loc)
    width = NB
    ident = jnp.eye(width, dtype=jnp.float32)
    row = lax.axis_index("row")
    col = lax.axis_index("col")
    last_row = lax.axis_size("row") - 1
    last_col = lax.axis_size("col") - 1
    top_mask = (row == 0).astype(jnp.float32)
    end_mask = (col == last_col).astype(jnp.float32)
    own_panel = amat[:, :width]
    own_strip = bmat[rows_loc - width :]
    zero = jnp.zeros((width, width), jnp.float32)
    small = jnp.stack(
        [
            jnp.where(col == 0, matmul(own_panel.T, own_panel), zero),
            jnp.where((col == 0) & (row == 0), own_panel[:width], zero),
            jnp.where(row == last_row, matmul(own_strip, own_strip.T), zero),
            jnp.where((col == last_col) & (row == last_row), own_strip[:, cols_loc - width :], zero),
        ]
    )
    small = lax.psum(small, ("row", "col"))
    own_panel, own_strip, small = lax.optimization_barrier((own_panel, own_strip, small))
    panel = broadcast(own_panel, "col", 0)
    strip = broadcast(own_strip, "row", last_row)
    left_inv = inverse_factor(small[0])
    right_inv = inverse_factor(small[2])
    vectors = matmul(panel, left_inv) + top_mask * jnp.pad(ident, ((0, rows_loc - width), (0, 0)))
    vectors_t = matmul(right_inv.T, strip) + end_mask * jnp.pad(
        ident, ((0, 0), (cols_loc - width, 0))
    )
    vectors, strip = lax.optimization_barrier((vectors, strip))
    products_a, products_b = lax.psum(
        (fast_matmul(vectors.T, amat), fast_matmul(vectors.T, bmat)), "row"
    )
    share = lax.psum_scatter(
        jnp.concatenate([fast_matmul(amat, vectors_t.T), fast_matmul(bmat, vectors_t.T)], axis=1),
        "col",
        scatter_dimension=0,
        tiled=True,
    )
    kinv_right = general_inverse(ident + matmul(right_inv.T, small[3]).T)
    kinv_left = general_inverse(ident + matmul(small[1], left_inv))
    scaled = jnp.concatenate(
        [matmul(share[:, :width], kinv_right.T), matmul(share[:, width:], kinv_right.T)], axis=1
    )
    gathered = lax.all_gather(scaled, "col", axis=0, tiled=True)
    cross = lax.psum(
        jnp.concatenate([matmul(products_a, vectors_t.T), matmul(products_b, vectors_t.T)], axis=0),
        "col",
    )

    def update(matrix, products, mixed, crossed):
        inner = products - matmul(matmul(crossed, kinv_right.T), vectors_t)
        low = jnp.concatenate([matmul(kinv_left, inner), vectors_t], axis=0)
        return matrix - fast_matmul(jnp.concatenate([vectors, mixed], axis=1), low)

    amat = update(amat, products_a, gathered[:, :width], cross[:width])
    bmat = update(bmat, products_b, gathered[:, width:], cross[width:])
    return (amat.reshape(1, rows_loc, 1, cols_loc), bmat.reshape(1, rows_loc, 1, cols_loc))


def solution(mesh):
    placed = (P("row", None, "col", None), P("row", None, "col", None))
    return jax.shard_map(
        on_device,
        mesh=mesh,
        in_specs=placed,
        out_specs=(P("row", None, "col", None), P("row", None, "col", None)),
        check_vma=False,
    )
```
